32 devices in a mesh: row: 4 (over y, x), col: 4 (over z), dep: 2 (over core).
Axes of the slice: x: 2, y: 2, z: 4, core: 2. Of those that a mesh axis runs over, the one named last changes fastest.
Arguments:
- matrix: float32 [16384, 16384], P('row', ('col', 'dep')), may hold values from -6 to 6
- vectors: float32 [64, 16384], P(None, ('row', 'col')), may hold values from -0.09375 to 0.09375
Outputs:
- reduced: float32 [16384, 16384], P('row', ('col', 'dep'))
The draws below stay inside these ranges and needn't reach their ends.
All inputs are finite; a program needn't handle non-finite values.
Results may differ from the reference program's by a relative error of at most 0.0001.
Values sent between devices are 32-bit elements; how exact they have to be, the bound alone decides.
A program may use at most 128 MiB of HBM per device.

```python
import jax
import jax.numpy as jnp
from jax import lax

N = 16384
B = 64


def levels(rng, shape, shards, least, largest):
    factor_of = 1.0
    for axis_at, parts in shards:
        draws = jax.random.uniform(jax.random.fold_in(jax.random.fold_in(rng, 6), axis_at), (parts,), jnp.float32, least / len(shards), largest / len(shards))
        factor_of = factor_of * jnp.repeat(jnp.exp(draws), shape[axis_at] // parts).reshape((-1,) + (1,) * (len(shape) - 1 - axis_at))
    return factor_of


def centred(own_key, extent, scale, limit, pieces=(), kind=jnp.bfloat16):
    loudness = levels(own_key, extent, pieces, -0.22, 0.18) if pieces else 1.0
    values = jax.random.normal(own_key, extent, jnp.float32) * scale * loudness
    return jnp.minimum(jnp.maximum(values, -limit), limit).astype(kind)


def setup_inputs(seed: int = 0) -> dict:
    splits = jax.random.split(jax.random.key(seed), 3)
    return {
        "matrix": centred(splits[0], (N, N), 1.0, 6.0, ((0, 4), (1, 8)), jnp.float32),
        "vectors": centred(splits[1], (B, N), (N // 4) ** -0.5, 0.09375, ((1, 16),), jnp.float32),
    }


highest = lax.Precision.HIGHEST


def contract(left, right, dims):
    return lax.dot_general(left, right, (dims, ((), ())), precision=highest)


def mask_vectors(values, first_row):
    panel_width, row_count = values.shape
    positions = first_row + lax.iota(jnp.int32, row_count)[None, :]
    reflector = lax.iota(jnp.int32, panel_width)[:, None]
    filler = jnp.where(positions == reflector + 1, 1.0, 0.0).astype(values.dtype)
    return jnp.where(positions > reflector + 1, values, filler)


def make_factor(gram):
    size_b = gram.shape[0]
    half_diag = 0.5 * jnp.diagonal(gram)
    scaled = jnp.triu(gram, 1) / half_diag[:, None]
    identity = jnp.eye(size_b, dtype=gram.dtype)
    inverse = identity - scaled
    powered = scaled
    for level in range((size_b - 1).bit_length() - 1):
        powered = jnp.dot(powered, powered, precision=highest)
        inverse = jnp.dot(inverse, identity + powered, precision=highest)
    return inverse / half_diag[None, :]


def reference(matrix, vectors):
    reflectors = mask_vectors(vectors, 0)
    gram = contract(reflectors, reflectors, ((1,), (1,)))
    factor = make_factor(gram)
    products = contract(reflectors, matrix, ((1,), (1,)))
    update = contract(factor, products, ((0,), (0,)))
    right_done = matrix - contract(update, reflectors, ((0,), (0,)))
    left_terms = contract(reflectors, right_done, ((1,), (0,)))
    scaled_terms = contract(factor, left_terms, ((0,), (0,)))
    return right_done - contract(reflectors, scaled_terms, ((0,), (0,)))
```

```python
import functools

import jax
import jax.numpy as jnp
from jax import lax
from jax.experimental import pallas as pl
from jax.experimental.pallas import tpu as pltpu
from jax.sharding import PartitionSpec as P

MESH = pl.DeviceIdType.MESH
highest = lax.Precision.HIGHEST
F32, BF16 = jnp.float32, jnp.bfloat16


def dot(a, b, dims=((1,), (0,)), precision=None):
    return lax.dot_general(a, b, (dims, ((), ())), precision=precision, preferred_element_type=F32)


def split(x):
    hi = x.astype(BF16)
    return hi, (x - hi.astype(F32)).astype(BF16)


def masked(values, first):
    pos = first + lax.broadcasted_iota(jnp.int32, values.shape, 1)
    ref = lax.broadcasted_iota(jnp.int32, values.shape, 0)
    filler = jnp.where(pos == ref + 1, 1.0, 0.0).astype(values.dtype)
    return jnp.where(pos > ref + 1, values, filler)


def make_factor(gram):
    size = gram.shape[0]
    i = lax.broadcasted_iota(jnp.int32, gram.shape, 0)
    j = lax.broadcasted_iota(jnp.int32, gram.shape, 1)
    identity = jnp.where(i == j, 1.0, 0.0).astype(F32)
    diag = gram * identity
    half_col = 0.5 * jnp.sum(diag, axis=1, keepdims=True)
    half_row = 0.5 * jnp.sum(diag, axis=0, keepdims=True)
    scaled = jnp.where(j > i, gram, 0.0) / half_col
    inverse = identity - scaled
    powered = scaled
    for _ in range((size - 1).bit_length() - 1):
        powered = dot(powered, powered, precision=highest)
        inverse = dot(inverse, identity + powered, precision=highest)
    return inverse / half_row


def exchange_kernel(R, C, D, m_ref, v_ref, lhs_ref, rhs_ref, mv, vraw, vrf, vhl, vcraw, vchl, zacc, zpart, zrecv,
                    ztot, ypart, ysib, yfl, yfr, ysr, ysl, yfull, gbuf, wdep, wcol, msem,
                    g_s, g_r, vg_sr, vg_sl, vg_r, vs_s, vs_r, vc_s, vc_r, zs_s, zs_r, za_s, za_r,
                    yb_s, yb_r, yr_s, yr_rl, yr_rr, yg_sr, yg_sl, yg_r, ya_s, ya_r, wd_s, wd_r, wc_s, wc_r):
    r, c, d = lax.axis_index("row"), lax.axis_index("col"), lax.axis_index("dep")
    rows, cols = m_ref.shape
    B = v_ref.shape[0] * v_ref.shape[1]
    rp = v_ref.shape[1]
    W = rows // C
    nb, wb = vcraw.shape[0], vcraw.shape[3]
    U = vc_s.shape[0]
    per_slab = U // (nb * D)
    ur = rp // per_slab

    for b in range(C):
        pltpu.make_async_copy(m_ref.at[pl.ds(b * W, W)], mv.at[pl.ds(b * W, W)], msem.at[b]).start()

    barrier = pltpu.get_barrier_semaphore()
    for axis, me, size in (("row", r, R), ("col", c, C), ("dep", d, D)):
        for k in range(1, size):
            pl.semaphore_signal(barrier, inc=1, device_id={axis: lax.rem(me + k, size)}, device_id_type=MESH)
    pl.semaphore_wait(barrier, R + C + D - 3)

    def rc(src, dst, ssem, rsem, axis, to):
        return pltpu.make_async_remote_copy(src_ref=src, dst_ref=dst, send_sem=ssem, recv_sem=rsem,
                                            device_id={axis: to}, device_id_type=MESH)

    def spread(buf, ssem, rsem, axis, me, size):
        for k in range(1, size):
            rc(buf.at[me], buf.at[me], ssem.at[k - 1], rsem.at[k - 1], axis, lax.rem(me + k, size)).start()

    def spread_wait(buf, ssem, rsem, axis, me, size):
        for k in range(1, size):
            got = buf.at[lax.rem(me + size - k, size)]
            rc(got, got, ssem.at[k - 1], rsem.at[k - 1], axis, lax.rem(me + k, size)).wait()

    def sib(buf, b, ssem, rsem):
        return [rc(buf.at[b, d], buf.at[b, d], ssem.at[k - 1, b], rsem.at[k - 1, b], "dep", lax.rem(d + k, D))
                for k in range(1, D)]

    def line_gather(buf, own, ssr, ssl, rs, sib_s, sib_r, send_own):
        def right(src, b):
            return rc(src, buf.at[b, d], ssr.at[b], rs.at[b], "col", lax.rem(c + 1, C))

        def left(src, b):
            return rc(src, buf.at[b, d], ssl.at[b], rs.at[b], "col", lax.rem(c + C - 1, C))

        @pl.when(c < C - 1)
        def _():
            right(own, c).start()

        @pl.when(c > 0)
        def _():
            left(own, c).start()

        if send_own:
            for cp in sib(buf, c, sib_s, sib_r):
                cp.start()
        for s in range(1, C):
            @pl.when(c - s >= 0)
            def _(s=s):
                b = c - s
                right(buf.at[b, d], b).wait_recv()

                @pl.when(c < C - 1)
                def _():
                    right(buf.at[b, d], b).start()
                for cp in sib(buf, b, sib_s, sib_r):
                    cp.start()

            @pl.when(c + s < C)
            def _(s=s):
                b = c + s
                left(buf.at[b, d], b).wait_recv()

                @pl.when(c > 0)
                def _():
                    left(buf.at[b, d], b).start()
                for cp in sib(buf, b, sib_s, sib_r):
                    cp.start()

        def drain():
            for b in range(C):
                @pl.when((c < C - 1) & (b <= c))
                def _(b=b):
                    right(buf.at[b, d], b).wait_send()

                @pl.when((c > 0) & (b >= c))
                def _(b=b):
                    left(buf.at[b, d], b).wait_send()

        def sib_wait(b):
            for k in range(1, D):
                got = buf.at[b, lax.rem(d + D - k, D)]
                rc(got, got, sib_s.at[k - 1, b], sib_r.at[k - 1, b], "dep", lax.rem(d + k, D)).wait()

        for b in range(C):
            if send_own:
                sib_wait(b)
            else:
                @pl.when(b != c)
                def _(b=b):
                    sib_wait(b)
        return drain

    vraw[c] = v_ref[...]
    vdrain = line_gather(vraw, v_ref.at[d], vg_sr, vg_sl, vg_r, vs_s, vs_r, False)

    colblk = c * D + d
    owner = (colblk * cols) // rows
    off = colblk * cols - owner * rows
    first_blk = off // W
    dist = lax.rem(r - owner + R, R)

    def unit(ref, u):
        slab, part = u // per_slab, u % per_slab
        return ref.at[slab // D, slab % D, pl.ds(part * ur, ur)]

    def vr_unit(u):
        slab, part = u // per_slab, u % per_slab
        if cols >= W:
            return vraw.at[first_blk + slab // D, slab % D, pl.ds(part * ur, ur)]
        return vraw.at[first_blk, slab % D, pl.ds(part * ur, ur), pl.ds(pl.multiple_of(off - first_blk * W, 128), cols)]

    def vc_copy(u, src, slot, delta):
        return rc(src, unit(vcraw, u), vc_s.at[u, slot], vc_r.at[u], "row", lax.rem(owner + delta, R))

    @pl.when(dist == 0)
    def _():
        for u in range(U):
            a = 1 + u % (R - 1)
            own_blk = vr_unit(u)
            vc_copy(u, own_blk, 0, a).start()
        for u in range(U):
            unit(vcraw, u)[...] = vr_unit(u)[...]

    for b in range(C):
        full = masked(vraw[b].reshape(B, W), r * rows + b * W)
        vrf[:, b * W:(b + 1) * W] = full
        hi, lo = split(full)
        vhl[0:B, b * W:(b + 1) * W] = hi
        vhl[B:2 * B, b * W:(b + 1) * W] = lo
    lhs_ref[B:2 * B, :] = vrf[...]
    gbuf[r] = dot(vrf[...], vrf[...], ((1,), (1,)), highest)
    spread(gbuf, g_s, g_r, "row", r, R)

    zacc[...] = jnp.zeros_like(zacc)
    t = min(256, W)
    for b in range(C):
        pltpu.make_async_copy(m_ref.at[pl.ds(b * W, W)], mv.at[pl.ds(b * W, W)], msem.at[b]).wait()

        @pl.loop(0, W // t)
        def _(i, b=b):
            at = pl.multiple_of(b * W + i * t, t)
            hi, lo = split(mv[pl.ds(at, t), :])
            v = vhl[:, pl.ds(at, t)]
            two = dot(v, hi)
            zacc[...] += two[0:B] + two[B:2 * B] + dot(v[0:B], lo)

    zr = B // R
    for i in range(R):
        zpart[i] = zacc[i * zr:(i + 1) * zr, :]
    for k in range(1, R):
        to = lax.rem(r + k, R)
        rc(zpart.at[to], zrecv.at[k - 1], zs_s.at[k - 1], zs_r.at[k - 1], "row", to).start()

    for u in range(U):
        a = 1 + u % (R - 1)

        @pl.when(dist == a)
        def _(u=u, a=a):
            vc_copy(u, unit(vcraw, u), 0, a).wait_recv()
            for k in range(1, R):
                if k != a:
                    vc_copy(u, unit(vcraw, u), k, k).start()
    for u in range(U):
        a = 1 + u % (R - 1)

        @pl.when((dist != 0) & (dist != a))
        def _(u=u, a=a):
            vc_copy(u, unit(vcraw, u), 0, a).wait_recv()
    for i in range(nb):
        full = masked(vcraw[i].reshape(B, wb), colblk * cols + i * wb)
        rhs_ref[0:B, i * wb:(i + 1) * wb] = full
        hi, lo = split(full)
        vchl[0:B, i * wb:(i + 1) * wb] = hi
        vchl[B:2 * B, i * wb:(i + 1) * wb] = lo

    order = sorted(range(C), key=lambda j: -abs(2 * j - (C - 1)))
    for j in order:
        @pl.loop(0, W // t)
        def _(i, j=j):
            hi, lo = split(mv[pl.ds(pl.multiple_of(j * W + i * t, t), t), :])
            v = vchl[...]
            two = dot(v, hi, ((1,), (1,)))
            y = two[0:B] + two[B:2 * B] + dot(v[0:B], lo, ((1,), (1,)))
            ypart[j, :, :, pl.ds(pl.multiple_of(i * t, t), t)] = y.reshape(D, rp, t)
        for k in range(1, D):
            to = lax.rem(d + k, D)
            rc(ypart.at[j, to], ysib.at[k - 1, j], yb_s.at[k - 1, j], yb_r.at[k - 1, j], "dep", to).start()

    for k in range(1, R):
        to = lax.rem(r + k, R)
        rc(zpart.at[to], zrecv.at[k - 1], zs_s.at[k - 1], zs_r.at[k - 1], "row", to).wait()
    total = zpart[r]
    for k in range(1, R):
        total = total + zrecv[k - 1]
    ztot[r] = total
    spread(ztot, za_s, za_r, "row", r, R)

    def ysum(j):
        acc = ypart[j, d]
        for k in range(1, D):
            acc = acc + ysib[k - 1, j]
        return acc

    for j in order:
        for k in range(1, D):
            to = lax.rem(d + k, D)
            rc(ypart.at[j, to], ysib.at[k - 1, j], yb_s.at[k - 1, j], yb_r.at[k - 1, j], "dep", to).wait()

    def red_right(j):
        return rc(ysr.at[j], yfl.at[j], yr_s.at[0, j], yr_rl.at[j], "col", lax.rem(c + 1, C))

    def red_left(j):
        return rc(ysl.at[j], yfr.at[j], yr_s.at[1, j], yr_rr.at[j], "col", lax.rem(c + C - 1, C))

    for s in range(C - 1):
        jr, jl = C - 1 - s, s

        @pl.when(c < jr)
        def _(j=jr):
            @pl.when(c == 0)
            def _():
                ysr[j] = ysum(j)

            @pl.when(c > 0)
            def _():
                red_right(j).wait_recv()
                ysr[j] = ysum(j) + yfl[j]
            red_right(j).start()

        @pl.when(c > jl)
        def _(j=jl):
            @pl.when(c == C - 1)
            def _():
                ysl[j] = ysum(j)

            @pl.when(c < C - 1)
            def _():
                red_left(j).wait_recv()
                ysl[j] = ysum(j) + yfr[j]
            red_left(j).start()

    yfull[c, d] = ysum(c)

    @pl.when(c > 0)
    def _():
        red_right(c).wait_recv()
        yfull[c, d] += yfl[c]

    @pl.when(c < C - 1)
    def _():
        red_left(c).wait_recv()
        yfull[c, d] += yfr[c]

    ydrain = line_gather(yfull, yfull.at[c, d], yg_sr, yg_sl, yg_r, ya_s, ya_r, True)

    spread_wait(gbuf, g_s, g_r, "row", r, R)
    gram = gbuf[0]
    for k in range(1, R):
        gram = gram + gbuf[k]
    factor_t = make_factor(gram).T
    spread_wait(ztot, za_s, za_r, "row", r, R)
    z = ztot[...].reshape(B, cols)
    vc = rhs_ref[0:B, :]
    wdep[d] = dot(z, vc, ((1,), (1,)), highest)
    spread(wdep, wd_s, wd_r, "dep", d, D)
    spread_wait(wdep, wd_s, wd_r, "dep", d, D)
    acc = wdep[0]
    for k in range(1, D):
        acc = acc + wdep[k]
    wcol[c] = acc
    spread(wcol, wc_s, wc_r, "col", c, C)
    for b in range(C):
        lhs_ref[0:B, b * W:(b + 1) * W] = dot(factor_t, yfull[b].reshape(B, W), precision=highest)
    spread_wait(wcol, wc_s, wc_r, "col", c, C)
    acc = wcol[0]
    for k in range(1, C):
        acc = acc + wcol[k]
    cross = dot(acc, factor_t, ((1,), (1,)), highest)
    left = z - dot(cross, vc, precision=highest)
    rhs_ref[B:2 * B, :] = dot(factor_t, left, precision=highest)

    vdrain()
    ydrain()
    for j in range(C):
        @pl.when(c < j)
        def _(j=j):
            red_right(j).wait_send()

        @pl.when(c > j)
        def _(j=j):
            red_left(j).wait_send()
    for u in range(U):
        a = 1 + u % (R - 1)

        @pl.when(dist == 0)
        def _(u=u, a=a):
            vc_copy(u, vr_unit(u), 0, a).wait_send()

        @pl.when(dist == a)
        def _(u=u, a=a):
            for k in range(1, R):
                if k != a:
                    vc_copy(u, unit(vcraw, u), k, k).wait_send()


def update_kernel(m_ref, lhs_ref, rhs_ref, out_ref, stack):
    @pl.when(pl.program_id(0) == 0)
    def _():
        hi, lo = split(rhs_ref[...])
        n = hi.shape[0]
        stack[0:n] = hi
        stack[n:2 * n] = hi
        stack[2 * n:3 * n] = lo

    hi, lo = split(lhs_ref[...].T)
    out_ref[...] = m_ref[...] - dot(jnp.concatenate([hi, lo, hi], axis=1), stack[...])


def solution(mesh):
    R, C, D = mesh.shape["row"], mesh.shape["col"], mesh.shape["dep"]

    def step(matrix, vectors):
        rows, cols = matrix.shape
        B, W = vectors.shape
        rp, zr = B // D, B // R
        nb, wb = max(1, cols // W), min(cols, W)
        ur = min(16, rp)
        units = nb * D * (rp // ur)
        dma, vm = pltpu.SemaphoreType.DMA, pltpu.VMEM
        lhs, rhs = pl.pallas_call(
            functools.partial(exchange_kernel, R, C, D),
            out_shape=(jax.ShapeDtypeStruct((2 * B, rows), F32), jax.ShapeDtypeStruct((2 * B, cols), F32)),
            in_specs=[pl.BlockSpec(memory_space=pl.ANY), pl.BlockSpec(memory_space=vm)],
            out_specs=[pl.BlockSpec(memory_space=vm)] * 2,
            scratch_shapes=[
                vm((rows, cols), F32), vm((C, D, rp, W), F32), vm((B, rows), F32), vm((2 * B, rows), BF16),
                vm((nb, D, rp, wb), F32), vm((2 * B, cols), BF16), vm((B, cols), F32), vm((R, zr, cols), F32),
                vm((R - 1, zr, cols), F32), vm((R, zr, cols), F32), vm((C, D, rp, W), F32),
                vm((D - 1, C, rp, W), F32), vm((C, rp, W), F32), vm((C, rp, W), F32), vm((C, rp, W), F32),
                vm((C, rp, W), F32), vm((C, D, rp, W), F32), vm((R, B, B), F32), vm((D, B, B), F32),
                vm((C, B, B), F32), dma((C,)),
                dma((R - 1,)), dma((R - 1,)), dma((C,)), dma((C,)), dma((C,)), dma((D - 1, C)), dma((D - 1, C)),
                dma((units, R)), dma((units,)), dma((R - 1,)), dma((R - 1,)), dma((R - 1,)), dma((R - 1,)),
                dma((D - 1, C)), dma((D - 1, C)), dma((2, C)), dma((C,)), dma((C,)), dma((C,)), dma((C,)), dma((C,)),
                dma((D - 1, C)), dma((D - 1, C)), dma((D - 1,)), dma((D - 1,)), dma((C - 1,)), dma((C - 1,)),
            ],
            compiler_params=pltpu.CompilerParams(collective_id=0, has_side_effects=True, vmem_limit_bytes=60 * 2**20),
            name="exchange",
        )(matrix, vectors.reshape(D, rp, W))
        rb = min(256, rows)
        return pl.pallas_call(
            update_kernel,
            grid=(rows // rb,),
            out_shape=jax.ShapeDtypeStruct((rows, cols), F32),
            in_specs=[
                pl.BlockSpec((rb, cols), lambda i: (i, 0)),
                pl.BlockSpec((2 * B, rb), lambda i: (0, i)),
                pl.BlockSpec((2 * B, cols), lambda i: (0, 0)),
            ],
            out_specs=pl.BlockSpec((rb, cols), lambda i: (i, 0)),
            scratch_shapes=[vm((6 * B, cols), BF16)],
            compiler_params=pltpu.CompilerParams(vmem_limit_bytes=40 * 2**20),
            name="update",
        )(matrix, lhs, rhs)

    return jax.shard_map(
        step, mesh=mesh, in_specs=(P("row", ("col", "dep")), P(None, ("row", "col"))),
        out_specs=P("row", ("col", "dep")), check_vma=False,
    )
```

```python
import functools

import jax
import jax.numpy as jnp
from jax import lax
from jax.experimental import pallas as pl
from jax.experimental.pallas import tpu as pltpu
from jax.sharding import PartitionSpec as P

MESH = pl.DeviceIdType.MESH
highest = lax.Precision.HIGHEST
F32, BF16 = jnp.float32, jnp.bfloat16


def dot(a, b, dims=((1,), (0,)), precision=None):
    return lax.dot_general(a, b, (dims, ((), ())), precision=precision, preferred_element_type=F32)


def split(x):
    hi = x.astype(BF16)
    return hi, (x - hi.astype(F32)).astype(BF16)


def masked(values, first):
    pos = first + lax.broadcasted_iota(jnp.int32, values.shape, 1)
    ref = lax.broadcasted_iota(jnp.int32, values.shape, 0)
    filler = jnp.where(pos == ref + 1, 1.0, 0.0).astype(values.dtype)
    return jnp.where(pos > ref + 1, values, filler)


def make_factor(gram):
    size = gram.shape[0]
    i = lax.broadcasted_iota(jnp.int32, gram.shape, 0)
    j = lax.broadcasted_iota(jnp.int32, gram.shape, 1)
    identity = jnp.where(i == j, 1.0, 0.0).astype(F32)
    diag = gram * identity
    half_col = 0.5 * jnp.sum(diag, axis=1, keepdims=True)
    half_row = 0.5 * jnp.sum(diag, axis=0, keepdims=True)
    scaled = jnp.where(j > i, gram, 0.0) / half_col
    inverse = identity - scaled
    powered = scaled
    for _ in range((size - 1).bit_length() - 1):
        powered = dot(powered, powered, precision=highest)
        inverse = dot(inverse, identity + powered, precision=highest)
    return inverse / half_row


def exchange_kernel(R, C, D, m_ref, v_ref, lhs_ref, rhs_ref, mv, vraw, vrf, vhl, vcraw, vchl, zacc, zpart, zrecv,
                    ztot, ypart, ysib, yfl, yfr, ysr, ysl, yfull, gbuf, wdep, wcol, msem,
                    g_s, g_r, vg_sr, vg_sl, vg_r, vs_s, vs_r, vc_s, vc_r, zs_s, zs_r, za_s, za_r,
                    yb_s, yb_r, yr_s, yr_rl, yr_rr, yg_sr, yg_sl, yg_r, ya_s, ya_r, wd_s, wd_r, wc_s, wc_r):
    r, c, d = lax.axis_index("row"), lax.axis_index("col"), lax.axis_index("dep")
    rows, cols = m_ref.shape
    B = v_ref.shape[0] * v_ref.shape[1]
    rp = v_ref.shape[1]
    W = rows // C
    nb, wb = vcraw.shape[0], vcraw.shape[3]
    U = vc_s.shape[0]
    per_slab = U // (nb * D)
    ur = rp // per_slab

    for b in range(C):
        pltpu.make_async_copy(m_ref.at[pl.ds(b * W, W)], mv.at[pl.ds(b * W, W)], msem.at[b]).start()

    barrier = pltpu.get_barrier_semaphore()
    for axis, me, size in (("row", r, R), ("col", c, C), ("dep", d, D)):
        for k in range(1, size):
            pl.semaphore_signal(barrier, inc=1, device_id={axis: lax.rem(me + k, size)}, device_id_type=MESH)
    pl.semaphore_wait(barrier, R + C + D - 3)

    def rc(src, dst, ssem, rsem, axis, to):
        return pltpu.make_async_remote_copy(src_ref=src, dst_ref=dst, send_sem=ssem, recv_sem=rsem,
                                            device_id={axis: to}, device_id_type=MESH)

    def spread(buf, ssem, rsem, axis, me, size):
        for k in range(1, size):
            rc(buf.at[me], buf.at[me], ssem.at[k - 1], rsem.at[k - 1], axis, lax.rem(me + k, size)).start()

    def spread_wait(buf, ssem, rsem, axis, me, size):
        for k in range(1, size):
            got = buf.at[lax.rem(me + size - k, size)]
            rc(got, got, ssem.at[k - 1], rsem.at[k - 1], axis, lax.rem(me + k, size)).wait()

    def sib(buf, b, ssem, rsem):
        return [rc(buf.at[b, d], buf.at[b, d], ssem.at[k - 1, b], rsem.at[k - 1, b], "dep", lax.rem(d + k, D))
                for k in range(1, D)]

    def line_gather(buf, own, ssr, ssl, rs, sib_s, sib_r, send_own):
        def right(src, b):
            return rc(src, buf.at[b, d], ssr.at[b], rs.at[b], "col", lax.rem(c + 1, C))

        def left(src, b):
            return rc(src, buf.at[b, d], ssl.at[b], rs.at[b], "col", lax.rem(c + C - 1, C))

        @pl.when(c < C - 1)
        def _():
            right(own, c).start()

        @pl.when(c > 0)
        def _():
            left(own, c).start()

        if send_own:
            for cp in sib(buf, c, sib_s, sib_r):
                cp.start()
        for s in range(1, C):
            @pl.when(c - s >= 0)
            def _(s=s):
                b = c - s
                right(buf.at[b, d], b).wait_recv()

                @pl.when(c < C - 1)
                def _():
                    right(buf.at[b, d], b).start()
                for cp in sib(buf, b, sib_s, sib_r):
                    cp.start()

            @pl.when(c + s < C)
            def _(s=s):
                b = c + s
                left(buf.at[b, d], b).wait_recv()

                @pl.when(c > 0)
                def _():
                    left(buf.at[b, d], b).start()
                for cp in sib(buf, b, sib_s, sib_r):
                    cp.start()

        def drain():
            for b in range(C):
                @pl.when((c < C - 1) & (b <= c))
                def _(b=b):
                    right(buf.at[b, d], b).wait_send()

                @pl.when((c > 0) & (b >= c))
                def _(b=b):
                    left(buf.at[b, d], b).wait_send()

        def sib_wait(b):
            for k in range(1, D):
                got = buf.at[b, lax.rem(d + D - k, D)]
                rc(got, got, sib_s.at[k - 1, b], sib_r.at[k - 1, b], "dep", lax.rem(d + k, D)).wait()

        for b in range(C):
            if send_own:
                sib_wait(b)
            else:
                @pl.when(b != c)
                def _(b=b):
                    sib_wait(b)
        return drain

    vraw[c] = v_ref[...]
    vdrain = line_gather(vraw, v_ref.at[d], vg_sr, vg_sl, vg_r, vs_s, vs_r, False)

    colblk = c * D + d
    owner = (colblk * cols) // rows
    off = colblk * cols - owner * rows
    first_blk = off // W
    dist = lax.rem(r - owner + R, R)

    def unit(ref, u):
        slab, part = u // per_slab, u % per_slab
        return ref.at[slab // D, slab % D, pl.ds(part * ur, ur)]

    def vr_unit(u):
        slab, part = u // per_slab, u % per_slab
        if cols >= W:
            return vraw.at[first_blk + slab // D, slab % D, pl.ds(part * ur, ur)]
        return vraw.at[first_blk, slab % D, pl.ds(part * ur, ur), pl.ds(pl.multiple_of(off - first_blk * W, 128), cols)]

    def vc_copy(u, src, slot, delta):
        return rc(src, unit(vcraw, u), vc_s.at[u, slot], vc_r.at[u], "row", lax.rem(owner + delta, R))

    @pl.when(dist == 0)
    def _():
        for u in range(U):
            a = 1 + u % (R - 1)
            own_blk = vr_unit(u)
            vc_copy(u, own_blk, 0, a).start()
        for u in range(U):
            unit(vcraw, u)[...] = vr_unit(u)[...]

    for b in range(C):
        full = masked(vraw[b].reshape(B, W), r * rows + b * W)
        vrf[:, b * W:(b + 1) * W] = full
        hi, lo = split(full)
        vhl[0:B, b * W:(b + 1) * W] = hi
        vhl[B:2 * B, b * W:(b + 1) * W] = lo
    lhs_ref[B:2 * B, :] = vrf[...]
    gbuf[r] = dot(vrf[...], vrf[...], ((1,), (1,)), highest)
    spread(gbuf, g_s, g_r, "row", r, R)

    zacc[...] = jnp.zeros_like(zacc)
    t = min(256, W)
    for b in range(C):
        pltpu.make_async_copy(m_ref.at[pl.ds(b * W, W)], mv.at[pl.ds(b * W, W)], msem.at[b]).wait()

        @pl.loop(0, W // t)
        def _(i, b=b):
            at = pl.multiple_of(b * W + i * t, t)
            hi, lo = split(mv[pl.ds(at, t), :])
            v = vhl[:, pl.ds(at, t)]
            two = dot(v, hi)
            zacc[...] += two[0:B] + two[B:2 * B] + dot(v[0:B], lo)

        if b == C // 2 - 1:
            for u in range(U):
                a = 1 + u % (R - 1)

                @pl.when(dist == a)
                def _(u=u, a=a):
                    vc_copy(u, unit(vcraw, u), 0, a).wait_recv()
                    for k in range(1, R):
                        if k != a:
                            vc_copy(u, unit(vcraw, u), k, k).start()

    zr = B // R
    for i in range(R):
        zpart[i] = zacc[i * zr:(i + 1) * zr, :]
    for k in range(1, R):
        to = lax.rem(r + k, R)
        rc(zpart.at[to], zrecv.at[k - 1], zs_s.at[k - 1], zs_r.at[k - 1], "row", to).start()

    for u in range(U):
        a = 1 + u % (R - 1)

        @pl.when((dist != 0) & (dist != a))
        def _(u=u, a=a):
            vc_copy(u, unit(vcraw, u), 0, a).wait_recv()
    for i in range(nb):
        full = masked(vcraw[i].reshape(B, wb), colblk * cols + i * wb)
        rhs_ref[0:B, i * wb:(i + 1) * wb] = full
        hi, lo = split(full)
        vchl[0:B, i * wb:(i + 1) * wb] = hi
        vchl[B:2 * B, i * wb:(i + 1) * wb] = lo

    order = sorted(range(C), key=lambda j: -abs(2 * j - (C - 1)))
    for j in order:
        @pl.loop(0, W // t)
        def _(i, j=j):
            hi, lo = split(mv[pl.ds(pl.multiple_of(j * W + i * t, t), t), :])
            v = vchl[...]
            two = dot(v, hi, ((1,), (1,)))
            y = two[0:B] + two[B:2 * B] + dot(v[0:B], lo, ((1,), (1,)))
            ypart[j, :, :, pl.ds(pl.multiple_of(i * t, t), t)] = y.reshape(D, rp, t)
        for k in range(1, D):
            to = lax.rem(d + k, D)
            rc(ypart.at[j, to], ysib.at[k - 1, j], yb_s.at[k - 1, j], yb_r.at[k - 1, j], "dep", to).start()

    for k in range(1, R):
        to = lax.rem(r + k, R)
        rc(zpart.at[to], zrecv.at[k - 1], zs_s.at[k - 1], zs_r.at[k - 1], "row", to).wait()
    total = zpart[r]
    for k in range(1, R):
        total = total + zrecv[k - 1]
    ztot[r] = total
    spread(ztot, za_s, za_r, "row", r, R)

    def ysum(j):
        acc = ypart[j, d]
        for k in range(1, D):
            acc = acc + ysib[k - 1, j]
        return acc

    for j in order:
        for k in range(1, D):
            to = lax.rem(d + k, D)
            rc(ypart.at[j, to], ysib.at[k - 1, j], yb_s.at[k - 1, j], yb_r.at[k - 1, j], "dep", to).wait()

    def red_right(j):
        return rc(ysr.at[j], yfl.at[j], yr_s.at[0, j], yr_rl.at[j], "col", lax.rem(c + 1, C))

    def red_left(j):
        return rc(ysl.at[j], yfr.at[j], yr_s.at[1, j], yr_rr.at[j], "col", lax.rem(c + C - 1, C))

    for s in range(C - 1):
        jr, jl = C - 1 - s, s

        @pl.when(c < jr)
        def _(j=jr):
            @pl.when(c == 0)
            def _():
                ysr[j] = ysum(j)

            @pl.when(c > 0)
            def _():
                red_right(j).wait_recv()
                ysr[j] = ysum(j) + yfl[j]
            red_right(j).start()

        @pl.when(c > jl)
        def _(j=jl):
            @pl.when(c == C - 1)
            def _():
                ysl[j] = ysum(j)

            @pl.when(c < C - 1)
            def _():
                red_left(j).wait_recv()
                ysl[j] = ysum(j) + yfr[j]
            red_left(j).start()

    yfull[c, d] = ysum(c)

    @pl.when(c > 0)
    def _():
        red_right(c).wait_recv()
        yfull[c, d] += yfl[c]

    @pl.when(c < C - 1)
    def _():
        red_left(c).wait_recv()
        yfull[c, d] += yfr[c]

    ydrain = line_gather(yfull, yfull.at[c, d], yg_sr, yg_sl, yg_r, ya_s, ya_r, True)

    spread_wait(gbuf, g_s, g_r, "row", r, R)
    gram = gbuf[0]
    for k in range(1, R):
        gram = gram + gbuf[k]
    factor_t = make_factor(gram).T
    spread_wait(ztot, za_s, za_r, "row", r, R)
    z = ztot[...].reshape(B, cols)
    vc = rhs_ref[0:B, :]
    wdep[d] = dot(z, vc, ((1,), (1,)), highest)
    spread(wdep, wd_s, wd_r, "dep", d, D)
    spread_wait(wdep, wd_s, wd_r, "dep", d, D)
    acc = wdep[0]
    for k in range(1, D):
        acc = acc + wdep[k]
    wcol[c] = acc
    spread(wcol, wc_s, wc_r, "col", c, C)
    for b in range(C):
        lhs_ref[0:B, b * W:(b + 1) * W] = dot(factor_t, yfull[b].reshape(B, W), precision=highest)
    spread_wait(wcol, wc_s, wc_r, "col", c, C)
    acc = wcol[0]
    for k in range(1, C):
        acc = acc + wcol[k]
    cross = dot(acc, factor_t, ((1,), (1,)), highest)
    left = z - dot(cross, vc, precision=highest)
    rhs_ref[B:2 * B, :] = dot(factor_t, left, precision=highest)

    vdrain()
    ydrain()
    for j in range(C):
        @pl.when(c < j)
        def _(j=j):
            red_right(j).wait_send()

        @pl.when(c > j)
        def _(j=j):
            red_left(j).wait_send()
    for u in range(U):
        a = 1 + u % (R - 1)

        @pl.when(dist == 0)
        def _(u=u, a=a):
            vc_copy(u, vr_unit(u), 0, a).wait_send()

        @pl.when(dist == a)
        def _(u=u, a=a):
            for k in range(1, R):
                if k != a:
                    vc_copy(u, unit(vcraw, u), k, k).wait_send()


def update_kernel(m_ref, lhs_ref, rhs_ref, out_ref, stack):
    @pl.when(pl.program_id(0) == 0)
    def _():
        hi, lo = split(rhs_ref[...])
        n = hi.shape[0]
        stack[0:n] = hi
        stack[n:2 * n] = hi
        stack[2 * n:3 * n] = lo

    hi, lo = split(lhs_ref[...].T)
    out_ref[...] = m_ref[...] - dot(jnp.concatenate([hi, lo, hi], axis=1), stack[...])


def solution(mesh):
    R, C, D = mesh.shape["row"], mesh.shape["col"], mesh.shape["dep"]

    def step(matrix, vectors):
        rows, cols = matrix.shape
        B, W = vectors.shape
        rp, zr = B // D, B // R
        nb, wb = max(1, cols // W), min(cols, W)
        ur = min(16, rp)
        units = nb * D * (rp // ur)
        dma, vm = pltpu.SemaphoreType.DMA, pltpu.VMEM
        lhs, rhs = pl.pallas_call(
            functools.partial(exchange_kernel, R, C, D),
            out_shape=(jax.ShapeDtypeStruct((2 * B, rows), F32), jax.ShapeDtypeStruct((2 * B, cols), F32)),
            in_specs=[pl.BlockSpec(memory_space=pl.ANY), pl.BlockSpec(memory_space=vm)],
            out_specs=[pl.BlockSpec(memory_space=vm)] * 2,
            scratch_shapes=[
                vm((rows, cols), F32), vm((C, D, rp, W), F32), vm((B, rows), F32), vm((2 * B, rows), BF16),
                vm((nb, D, rp, wb), F32), vm((2 * B, cols), BF16), vm((B, cols), F32), vm((R, zr, cols), F32),
                vm((R - 1, zr, cols), F32), vm((R, zr, cols), F32), vm((C, D, rp, W), F32),
                vm((D - 1, C, rp, W), F32), vm((C, rp, W), F32), vm((C, rp, W), F32), vm((C, rp, W), F32),
                vm((C, rp, W), F32), vm((C, D, rp, W), F32), vm((R, B, B), F32), vm((D, B, B), F32),
                vm((C, B, B), F32), dma((C,)),
                dma((R - 1,)), dma((R - 1,)), dma((C,)), dma((C,)), dma((C,)), dma((D - 1, C)), dma((D - 1, C)),
                dma((units, R)), dma((units,)), dma((R - 1,)), dma((R - 1,)), dma((R - 1,)), dma((R - 1,)),
                dma((D - 1, C)), dma((D - 1, C)), dma((2, C)), dma((C,)), dma((C,)), dma((C,)), dma((C,)), dma((C,)),
                dma((D - 1, C)), dma((D - 1, C)), dma((D - 1,)), dma((D - 1,)), dma((C - 1,)), dma((C - 1,)),
            ],
            compiler_params=pltpu.CompilerParams(collective_id=0, has_side_effects=True, vmem_limit_bytes=60 * 2**20),
            name="exchange",
        )(matrix, vectors.reshape(D, rp, W))
        rb = min(512, rows)
        return pl.pallas_call(
            update_kernel,
            grid=(rows // rb,),
            out_shape=jax.ShapeDtypeStruct((rows, cols), F32),
            in_specs=[
                pl.BlockSpec((rb, cols), lambda i: (i, 0)),
                pl.BlockSpec((2 * B, rb), lambda i: (0, i)),
                pl.BlockSpec((2 * B, cols), lambda i: (0, 0)),
            ],
            out_specs=pl.BlockSpec((rb, cols), lambda i: (i, 0)),
            scratch_shapes=[vm((6 * B, cols), BF16)],
            compiler_params=pltpu.CompilerParams(vmem_limit_bytes=40 * 2**20),
            name="update",
        )(matrix, lhs, rhs)

    return jax.shard_map(
        step, mesh=mesh, in_specs=(P("row", ("col", "dep")), P(None, ("row", "col"))),
        out_specs=P("row", ("col", "dep")), check_vma=False,
    )
```
